32 devices in a mesh: dp: 1 (over z), tp: 4 (over y), ctx: 8 (over x, core).
Axes of the slice: x: 4, y: 4, z: 1, core: 2. Of those that a mesh axis runs over, the one named last changes fastest.
The devices are a block of a 4x4x8 slice.
Arguments:
- hidden: bfloat16 [1024, 8192], P(('dp', 'ctx'))
- w_q: bfloat16 [8192, 8192], P(None, 'tp')
- w_k: bfloat16 [8192, 1024], P(None, 'tp')
- w_v: bfloat16 [8192, 1024], P(None, 'tp')
- w_o: bfloat16 [8192, 8192], P('tp')
- k_prefix: bfloat16 [2048, 8, 128], P(('dp', 'ctx'), 'tp')
- v_prefix: bfloat16 [2048, 8, 128], P(('dp', 'ctx'), 'tp')
- k_suffix: bfloat16 [1024, 256, 8, 128], P(('dp', 'ctx'), None, 'tp')
- v_suffix: bfloat16 [1024, 256, 8, 128], P(('dp', 'ctx'), None, 'tp')
- seq_lens: int32 [1024], P(('dp', 'ctx'))
Outputs:
- output: bfloat16 [1024, 8192], P(('dp', 'ctx'))
All inputs are finite; a program needn't handle non-finite values.
Results may differ from the reference program's by a relative error of at most 0.00452208.
Values are sent between devices in bfloat16 or wider.
A program may use at most 768 MiB of HBM per device.

```python
import math
import jax
import jax.numpy as jnp
from jax import lax

NUM_SEQS = 1024
PREFIX_LEN = 2048
SUFFIX_LEN = 256
MODEL_DIM = 8192
NUM_HEADS = 64
KV_HEADS = 8
HEAD_DIM = 128
GROUP_SIZE = NUM_HEADS // KV_HEADS


def setup_inputs(seed: int = 0, part: int = 0) -> dict:
    root_key = jax.random.key(seed)
    part_key = jax.random.fold_in(root_key, part)
    weight_keys = jax.random.split(root_key, 4)
    draw_keys = jax.random.split(part_key, 10)
    topic_count = 16
    log_ratio = min(max(math.log(2.0 * PREFIX_LEN / (topic_count * SUFFIX_LEN)), -3.0), 3.0)
    amp_prefix = 2.0 + max(-log_ratio, 0.0)
    amp_suffix = 3.0 + max(log_ratio, 0.0)
    q_cols = NUM_HEADS * HEAD_DIM
    kv_cols = KV_HEADS * HEAD_DIM
    in_scale = MODEL_DIM ** -0.5
    w_q = jax.random.normal(weight_keys[0], (MODEL_DIM, q_cols), jnp.float32) * in_scale
    lead_cols = w_q.reshape(MODEL_DIM, KV_HEADS, GROUP_SIZE, HEAD_DIM)[:, :, 0, :].reshape(MODEL_DIM, kv_cols)
    w_k = 0.6 * lead_cols + 0.8 * in_scale * jax.random.normal(weight_keys[1], (MODEL_DIM, kv_cols), jnp.float32)
    w_v = in_scale * jax.random.normal(weight_keys[2], (MODEL_DIM, kv_cols), jnp.float32)
    w_o = jax.random.normal(weight_keys[3], (q_cols, MODEL_DIM), jnp.float32) * q_cols ** -0.5
    hidden = jax.random.normal(draw_keys[0], (NUM_SEQS, MODEL_DIM), jnp.float32)
    topic_hid = jax.random.normal(draw_keys[1], (topic_count, MODEL_DIM), jnp.float32)
    topic_key = jnp.dot(topic_hid, w_k).reshape(topic_count, KV_HEADS, HEAD_DIM)
    topic_val = jnp.dot(topic_hid, w_v).reshape(topic_count, KV_HEADS, HEAD_DIM)
    pos_topic = jnp.arange(PREFIX_LEN) * topic_count // PREFIX_LEN
    kv_shape = (PREFIX_LEN, KV_HEADS, HEAD_DIM)
    k_prefix = amp_prefix * topic_key[pos_topic] + jax.random.normal(draw_keys[2], kv_shape, jnp.float32)
    v_prefix = topic_val[pos_topic] + 0.5 * jax.random.normal(draw_keys[3], kv_shape, jnp.float32)
    own_hid = jax.random.normal(draw_keys[4], (NUM_SEQS, MODEL_DIM), jnp.float32)
    stale_hid = jax.random.normal(draw_keys[5], (NUM_SEQS, MODEL_DIM), jnp.float32)
    head_shape = (NUM_SEQS, 1, KV_HEADS, HEAD_DIM)
    own_key = jnp.dot(own_hid, w_k).reshape(head_shape)
    own_val = jnp.dot(own_hid, w_v).reshape(head_shape)
    stale_key = jnp.dot(stale_hid, w_k).reshape(head_shape)
    stale_val = jnp.dot(stale_hid, w_v).reshape(head_shape)
    seq_lens = jax.random.randint(draw_keys[6], (NUM_SEQS,), 0, SUFFIX_LEN)
    seq_lens = seq_lens.at[0].set(SUFFIX_LEN - 1).at[NUM_SEQS - 1].set(0)
    in_use = (jnp.arange(SUFFIX_LEN)[None, :] < seq_lens[:, None])[:, :, None, None]
    suf_shape = (NUM_SEQS, SUFFIX_LEN, KV_HEADS, HEAD_DIM)
    k_suffix = amp_suffix * jnp.where(in_use, own_key, stale_key) + jax.random.normal(draw_keys[7], suf_shape, jnp.float32)
    v_suffix = jnp.where(in_use, own_val, stale_val) + 0.5 * jax.random.normal(draw_keys[8], suf_shape, jnp.float32)
    return dict(hidden=hidden.astype(jnp.bfloat16), w_q=w_q.astype(jnp.bfloat16), w_k=w_k.astype(jnp.bfloat16), w_v=w_v.astype(jnp.bfloat16), w_o=w_o.astype(jnp.bfloat16), k_prefix=k_prefix.astype(jnp.bfloat16), v_prefix=v_prefix.astype(jnp.bfloat16), k_suffix=k_suffix.astype(jnp.bfloat16), v_suffix=v_suffix.astype(jnp.bfloat16), seq_lens=seq_lens)


def reference(hidden, w_q, w_k, w_v, w_o, k_prefix, v_prefix, k_suffix, v_suffix, seq_lens):
    q_all = jnp.dot(hidden, w_q, preferred_element_type=jnp.float32).astype(jnp.bfloat16)
    k_new = jnp.dot(hidden, w_k, preferred_element_type=jnp.float32).astype(jnp.bfloat16)
    v_new = jnp.dot(hidden, w_v, preferred_element_type=jnp.float32).astype(jnp.bfloat16)
    slot_ids = jnp.arange(SUFFIX_LEN)
    at_new = (slot_ids[None, :] == seq_lens[:, None])[:, :, None, None]
    k_cur = jnp.where(at_new, k_new.reshape(NUM_SEQS, 1, KV_HEADS, HEAD_DIM), k_suffix).astype(jnp.float32)
    v_cur = jnp.where(at_new, v_new.reshape(NUM_SEQS, 1, KV_HEADS, HEAD_DIM), v_suffix).astype(jnp.float32)
    visible = slot_ids[None, :] <= seq_lens[:, None]
    q_grp = q_all.astype(jnp.float32).reshape(NUM_SEQS, KV_HEADS, GROUP_SIZE, HEAD_DIM)
    k_pre32 = k_prefix.astype(jnp.float32)
    v_pre32 = v_prefix.astype(jnp.float32)
    score_scale = HEAD_DIM ** -0.5

    def one_sequence(seq_items):
        q_one, k_one, v_one, vis_one = seq_items
        s_pre = jnp.einsum('kgd,pkd->kgp', q_one, k_pre32) * score_scale
        s_suf = jnp.einsum('kgd,skd->kgs', q_one, k_one) * score_scale
        s_suf = jnp.where(vis_one[None, None, :], s_suf, -jnp.inf)
        run_max = jnp.maximum(jnp.max(s_pre, axis=-1), jnp.max(s_suf, axis=-1))[..., None]
        e_pre = jnp.exp(s_pre - run_max)
        e_suf = jnp.exp(s_suf - run_max)
        weight_sum = jnp.sum(e_pre, axis=-1) + jnp.sum(e_suf, axis=-1)
        weighted = jnp.einsum('kgp,pkd->kgd', e_pre, v_pre32) + jnp.einsum('kgs,skd->kgd', e_suf, v_one)
        return weighted / weight_sum[..., None]

    attn_out = lax.map(one_sequence, (q_grp, k_cur, v_cur, visible))
    attn_out = attn_out.reshape(NUM_SEQS, NUM_HEADS * HEAD_DIM).astype(jnp.bfloat16)
    out_hidden = hidden.astype(jnp.float32) + jnp.dot(attn_out, w_o, preferred_element_type=jnp.float32)
    return out_hidden.astype(jnp.bfloat16)
```

```python
import functools
import math

import jax
import jax.numpy as jnp
from jax import lax
from jax.experimental import pallas as pl
from jax.experimental.pallas import tpu as pltpu
from jax.sharding import PartitionSpec as P

MESH = pl.DeviceIdType.MESH
F32, BF16 = jnp.float32, jnp.bfloat16


def qkv_gather_kernel(x_ref, kvp_ref, wq_ref, wk_ref, wv_ref, qkv_ref, all_ref, wbuf, wsem, send_sem, recv_sem, pair_send, pair_recv):
    n_ctx = all_ref.shape[0]
    me = lax.axis_index('ctx')
    right, left = lax.rem(me + 2, n_ctx), lax.rem(me + n_ctx - 2, n_ctx)
    far = lax.rem(me + 4, n_ctx)
    partner = me + 1 - 2 * lax.rem(me, 2)
    depth, width = wk_ref.shape
    q_blocks = wq_ref.shape[1] // width
    blocks = q_blocks + 2
    bufs = wbuf.shape[0]

    def fetch(j):
        slot = lax.rem(j, bufs)

        @pl.when(j < q_blocks)
        def _():
            columns = pl.ds(pl.multiple_of(j * width, width), width)
            pltpu.make_async_copy(wq_ref.at[:, columns], wbuf.at[slot], wsem.at[slot]).start()

        @pl.when(j == q_blocks)
        def _():
            pltpu.make_async_copy(wk_ref, wbuf.at[slot], wsem.at[slot]).start()

        @pl.when(j == q_blocks + 1)
        def _():
            pltpu.make_async_copy(wv_ref, wbuf.at[slot], wsem.at[slot]).start()

    for j in range(bufs):
        fetch(jnp.int32(j))

    barrier = pltpu.get_barrier_semaphore()
    for peer in (left, right, partner):
        pl.semaphore_signal(barrier, inc=1, device_id={'ctx': peer}, device_id_type=MESH)
    pl.semaphore_wait(barrier, 3)

    def send(src, dst, index, peer):
        return pltpu.make_async_remote_copy(src_ref=src, dst_ref=dst, send_sem=send_sem.at[index], recv_sem=recv_sem.at[index], device_id={'ctx': peer}, device_id_type=MESH)

    def to_partner(slot, index):
        src = kvp_ref if slot is None else all_ref.at[slot]
        dst = all_ref.at[me if slot is None else slot]
        return pltpu.make_async_remote_copy(src_ref=src, dst_ref=dst, send_sem=pair_send.at[index], recv_sem=pair_recv.at[index], device_id={'ctx': partner}, device_id_type=MESH)

    go_right = send(kvp_ref, all_ref.at[me], 0, right)
    go_left = send(kvp_ref, all_ref.at[me], 1, left)
    go_right.start()
    go_left.start()
    own_pair = to_partner(None, 0)
    own_pair.start()
    all_ref[me] = kvp_ref[...]

    def project(j, carry):
        slot = lax.rem(j, bufs)
        pltpu.make_async_copy(wk_ref, wbuf.at[slot], wsem.at[slot]).wait()
        qkv_ref[j] = jnp.dot(x_ref[...], wbuf[slot], preferred_element_type=F32).astype(BF16)
        fetch(j + bufs)
        return carry

    split = min(7, blocks - 2)
    lax.fori_loop(0, split, project, 0)

    send(kvp_ref, all_ref.at[left], 0, right).wait_recv()
    on_right = send(all_ref.at[left, 0], all_ref.at[left, 0], 2, right)
    on_right.start()
    send(kvp_ref, all_ref.at[right], 1, left).wait_recv()
    on_left = send(all_ref.at[right, 1], all_ref.at[right, 1], 3, left)
    on_left.start()
    left_pair = to_partner(left, 1)
    left_pair.start()
    right_pair = to_partner(right, 2)
    right_pair.start()

    lax.fori_loop(split, blocks, project, 0)

    send(all_ref.at[far, 0], all_ref.at[far, 0], 2, right).wait_recv()
    send(all_ref.at[far, 1], all_ref.at[far, 1], 3, left).wait_recv()
    far_pair = to_partner(far, 3)
    far_pair.start()
    for copy in (go_right, go_left, on_right, on_left):
        copy.wait_send()
    for copy in (own_pair, left_pair, right_pair, far_pair):
        copy.wait_send()
    shift = partner - me
    for index, slot in enumerate((me, left, right, far)):
        landed = all_ref.at[slot + shift]
        pltpu.make_async_remote_copy(src_ref=landed, dst_ref=landed, send_sem=pair_send.at[index], recv_sem=pair_recv.at[index], device_id={'ctx': partner}, device_id_type=MESH).wait_recv()


def attention_kernel(scale, len_ref, qa_ref, kn_ref, vn_ref, qb_ref, ks_ref, vs_ref, kvp_ref, out_ref, o_suf, m_suf, l_suf):
    seqs, kv_heads, group, dim = out_ref.shape
    rows = kv_heads * group
    slots = ks_ref.shape[1]
    first = pl.program_id(0) * seqs
    sub = min(8, seqs)
    factor = scale * math.log2(math.e)
    dims = (((1,), (1,)), ((), ()))

    column = lax.broadcasted_iota(jnp.int32, (rows, slots), 1)
    head = lax.broadcasted_iota(jnp.int32, (rows, slots), 0) // group
    place = jnp.where(lax.rem(column, kv_heads) == head, column // kv_heads, slots)

    def suffix(i, carry):
        span = pl.ds(pl.multiple_of(i * sub * rows, sub * rows), sub * rows)
        scores = []
        for s in range(sub):
            q_one = qa_ref[pl.ds(pl.multiple_of((i * sub + s) * rows, rows), rows)]
            one = lax.dot_general(q_one, ks_ref[i * sub + s], dims, preferred_element_type=F32)
            scores.append(jnp.where(place < len_ref[first + i * sub + s], one, -jnp.inf))
        scores = jnp.concatenate(scores, axis=0)
        own = jnp.sum(qa_ref[span].astype(F32) * kn_ref[span].astype(F32), axis=-1, keepdims=True)
        top = jnp.maximum(jnp.max(scores, axis=-1, keepdims=True), own)
        e = jnp.exp2((scores - top) * factor)
        e_own = jnp.exp2((own - top) * factor)
        total = jnp.sum(e, axis=-1, keepdims=True) + e_own
        e = e.astype(BF16)
        o = [jnp.dot(e[s * rows:(s + 1) * rows], vs_ref[i * sub + s], preferred_element_type=F32) for s in range(sub)]
        o = jnp.concatenate(o, axis=0) + e_own * vn_ref[span].astype(F32)
        block = pl.ds(i * sub, sub)
        o_suf[block] = o.reshape(sub, kv_heads, group, dim)
        m_suf[block] = top.reshape(sub, kv_heads, group, 1)
        l_suf[block] = total.reshape(sub, kv_heads, group, 1)
        return carry

    lax.fori_loop(0, seqs // sub, suffix, 0)

    for kv in range(kv_heads):
        keys = kvp_ref[:, 0, kv].reshape(-1, dim)
        values = kvp_ref[:, 1, kv].reshape(-1, dim)
        s = lax.dot_general(qb_ref[kv], keys, dims, preferred_element_type=F32)
        top_pre = jnp.max(s, axis=-1, keepdims=True)
        e = jnp.exp2((s - top_pre) * factor)
        total_pre = jnp.sum(e, axis=-1, keepdims=True)
        o_pre = jnp.dot(e.astype(BF16), values, preferred_element_type=F32)
        top_suf = m_suf[:, kv].reshape(seqs * group, 1)
        top = jnp.maximum(top_pre, top_suf)
        w_pre = jnp.exp2((top_pre - top) * factor)
        w_suf = jnp.exp2((top_suf - top) * factor)
        total = w_pre * total_pre + w_suf * l_suf[:, kv].reshape(seqs * group, 1)
        o = (w_pre * o_pre + w_suf * o_suf[:, kv].reshape(seqs * group, dim)) / total
        out_ref[:, kv] = o.reshape(seqs, group, dim).astype(BF16)


ORDER = ((2, 0), (2, 1), (1, 0), (3, 1), (1, 1), (3, 0), (0, 0), (0, 1))


def project_reduce_kernel(n_tp, pieces, att_ref, x_ref, wo_ref, y_ref, wbuf, part, first_in, direct_in, sum_in, wsem, send_sem, recv_sem):
    me = lax.axis_index('tp')
    right, left = lax.rem(me + 1, n_tp), lax.rem(me + n_tp - 1, n_tp)
    rows = att_ref.shape[0]
    half = wbuf.shape[2]
    bufs = wbuf.shape[0]
    step = rows // pieces

    def columns(owner, which, width):
        return pl.ds(pl.multiple_of((owner * 2 + which) * half, half), width)

    def weights(k):
        away, which = ORDER[k]
        return pltpu.make_async_copy(wo_ref.at[:, columns(lax.rem(me + away, n_tp), which, half)], wbuf.at[k % bufs], wsem.at[k % bufs])

    for k in range(bufs):
        weights(k).start()

    barrier = pltpu.get_barrier_semaphore()
    for peer in (left, right):
        pl.semaphore_signal(barrier, inc=1, device_id={'tp': peer}, device_id_type=MESH)
    pl.semaphore_wait(barrier, 2)

    def copy(kind, way, p, src, dst):
        return pltpu.make_async_remote_copy(src_ref=src, dst_ref=dst, send_sem=send_sem.at[kind, way, p], recv_sem=recv_sem.at[kind, way, p], device_id={'tp': (right, left)[way]}, device_id_type=MESH)

    def span(p):
        return pl.ds(p * step, step)

    started = []

    def launch(*args):
        one = copy(*args)
        one.start()
        started.append(one)

    def compute(k):
        weights(k).wait()
        part[k] = jnp.dot(att_ref[...], wbuf[k % bufs], preferred_element_type=F32)
        if k + bufs < len(ORDER):
            weights(k + bufs).start()

    compute(0)
    for p in range(pieces):
        launch(0, 1, p, part.at[0, span(p)], first_in.at[1, span(p)])
    compute(1)
    for p in range(pieces):
        launch(0, 0, p, part.at[1, span(p)], first_in.at[0, span(p)])
    compute(2)
    for p in range(pieces):
        launch(1, 0, p, part.at[2, span(p)], direct_in.at[0, span(p)])
    compute(3)
    for p in range(pieces):
        launch(1, 1, p, part.at[3, span(p)], direct_in.at[1, span(p)])
    for k in range(4, 8):
        compute(k)
    for p in range(pieces):
        for way, k in ((0, 4), (1, 5)):
            copy(0, way, p, first_in.at[way, span(p)], first_in.at[way, span(p)]).wait_recv()
            part[k, span(p)] += first_in[way, span(p)]
            launch(2, way, p, part.at[k, span(p)], sum_in.at[way, span(p)])
    mine = columns(me, 0, 2 * half)
    for p in range(pieces):
        for way in (0, 1):
            copy(1, way, p, direct_in.at[way, span(p)], direct_in.at[way, span(p)]).wait_recv()
            copy(2, way, p, sum_in.at[way, span(p)], sum_in.at[way, span(p)]).wait_recv()
        for which in (0, 1):
            total = part[6 + which, span(p)] + sum_in[1 - which, span(p)] + direct_in[which, span(p)]
            total = total + x_ref[span(p), columns(me, which, half)].astype(F32)
            y_ref[span(p), columns(me, which, half)] = total.astype(BF16)
        for way in (0, 1):
            launch(3, way, p, y_ref.at[span(p), mine], y_ref.at[span(p), mine])
    for p in range(pieces):
        for way, source in ((0, left), (1, right)):
            block = y_ref.at[span(p), columns(source, 0, 2 * half)]
            copy(3, way, p, block, block).wait_recv()
            block = y_ref.at[span(p), columns(source, way, half)]
            launch(4, way, p, block, block)
    far = lax.rem(me + 2, n_tp)
    for p in range(pieces):
        for way in (0, 1):
            block = y_ref.at[span(p), columns(far, way, half)]
            copy(4, way, p, block, block).wait_recv()
    for one in started:
        one.wait_send()


def solution(mesh):
    n_ctx, n_tp = mesh.shape['ctx'], mesh.shape['tp']
    row_axes = ('dp', 'ctx')
    vmem = pl.BlockSpec(memory_space=pltpu.VMEM)
    hbm = pl.BlockSpec(memory_space=pl.ANY)
    limit = 60 * 1024 * 1024

    def device_step(hidden, w_q, w_k, w_v, w_o, k_prefix, v_prefix, k_suffix, v_suffix, seq_lens):
        seqs, model = hidden.shape
        positions, kv_heads, dim = k_prefix.shape
        slots = k_suffix.shape[1]
        group = w_q.shape[1] // (kv_heads * dim)
        heads = kv_heads * group
        width = w_k.shape[1]
        blocks = w_q.shape[1] // width + 2

        kv_own = jnp.stack([k_prefix, v_prefix]).transpose(0, 2, 1, 3)
        qkv, kv_all = pl.pallas_call(
            qkv_gather_kernel,
            name='qkv_gather',
            out_shape=(jax.ShapeDtypeStruct((blocks, seqs, width), BF16), jax.ShapeDtypeStruct((n_ctx, 2, kv_heads, positions, dim), BF16)),
            in_specs=[vmem, vmem, hbm, hbm, hbm],
            out_specs=(vmem, vmem),
            scratch_shapes=[pltpu.VMEM((4, model, width), BF16), pltpu.SemaphoreType.DMA((4,)), pltpu.SemaphoreType.DMA((4,)), pltpu.SemaphoreType.DMA((4,)), pltpu.SemaphoreType.DMA((4,)), pltpu.SemaphoreType.DMA((4,))],
            compiler_params=pltpu.CompilerParams(collective_id=0, has_side_effects=True, vmem_limit_bytes=limit),
        )(hidden, kv_own, w_q, w_k, w_v)

        per = width // dim
        q = qkv[:blocks - 2].reshape(blocks - 2, seqs, per, dim)
        q_rows = q.transpose(1, 0, 2, 3).reshape(seqs * heads, dim)
        q_heads = q_rows.reshape(seqs, kv_heads, group, dim).transpose(1, 0, 2, 3).reshape(kv_heads, seqs * group, dim)
        k_new, v_new = (jnp.broadcast_to(a.reshape(seqs, kv_heads, 1, dim), (seqs, kv_heads, group, dim)).reshape(seqs * heads, dim) for a in (qkv[blocks - 2], qkv[blocks - 1]))

        nb = min(32, seqs)
        row_spec = pl.BlockSpec((nb * heads, dim), lambda i, lens: (i, 0))
        cache_spec = pl.BlockSpec((nb, slots * kv_heads, dim), lambda i, lens: (i, 0, 0))
        att = pl.pallas_call(
            functools.partial(attention_kernel, dim ** -0.5),
            name='attention',
            out_shape=jax.ShapeDtypeStruct((seqs, kv_heads, group, dim), BF16),
            grid_spec=pltpu.PrefetchScalarGridSpec(
                num_scalar_prefetch=1,
                grid=(seqs // nb,),
                in_specs=[row_spec, row_spec, row_spec, pl.BlockSpec((kv_heads, nb * group, dim), lambda i, lens: (0, i, 0)), cache_spec, cache_spec, pl.BlockSpec((n_ctx, 2, kv_heads, positions, dim), lambda i, lens: (0, 0, 0, 0, 0))],
                out_specs=pl.BlockSpec((nb, kv_heads, group, dim), lambda i, lens: (i, 0, 0, 0)),
                scratch_shapes=[pltpu.VMEM((nb, kv_heads, group, dim), F32), pltpu.VMEM((nb, kv_heads, group, 1), F32), pltpu.VMEM((nb, kv_heads, group, 1), F32)],
            ),
            compiler_params=pltpu.CompilerParams(vmem_limit_bytes=limit),
        )(seq_lens, q_rows, k_new, v_new, q_heads, k_suffix.reshape(seqs, slots * kv_heads, dim), v_suffix.reshape(seqs, slots * kv_heads, dim), kv_all)
        att = att.reshape(seqs, heads * dim)

        half = model // (2 * n_tp)
        pieces = 4
        return pl.pallas_call(
            functools.partial(project_reduce_kernel, n_tp, pieces),
            name='project_reduce',
            out_shape=jax.ShapeDtypeStruct((seqs, model), BF16),
            in_specs=[vmem, vmem, hbm],
            out_specs=vmem,
            scratch_shapes=[
                pltpu.VMEM((3, heads * dim, half), BF16),
                pltpu.VMEM((8, seqs, half), F32),
                pltpu.VMEM((2, seqs, half), F32),
                pltpu.VMEM((2, seqs, half), F32),
                pltpu.VMEM((2, seqs, half), F32),
                pltpu.SemaphoreType.DMA((3,)),
                pltpu.SemaphoreType.DMA((5, 2, pieces)),
                pltpu.SemaphoreType.DMA((5, 2, pieces)),
            ],
            compiler_params=pltpu.CompilerParams(collective_id=1, has_side_effects=True, vmem_limit_bytes=limit),
        )(att, hidden, w_o)

    spec_in = (P(row_axes, None), P(None, 'tp'), P(None, 'tp'), P(None, 'tp'), P('tp', None), P(row_axes, 'tp', None), P(row_axes, 'tp', None), P(row_axes, None, 'tp', None), P(row_axes, None, 'tp', None), P(row_axes))
    return jax.shard_map(device_step, mesh=mesh, in_specs=spec_in, out_specs=P(row_axes, None), check_vma=False)
```

```python
import functools
import math

import jax
import jax.numpy as jnp
from jax import lax
from jax.experimental import pallas as pl
from jax.experimental.pallas import tpu as pltpu
from jax.sharding import PartitionSpec as P

MESH = pl.DeviceIdType.MESH
F32, BF16 = jnp.float32, jnp.bfloat16
LAST = (((1,), (1,)), ((), ()))

ORDER = ((2, 0), (2, 1), (1, 0), (3, 1), (1, 1), (3, 0), (0, 0), (0, 1))
SUB = 8
DEPTH = 3
PREFIX = 32
CHUNKS = 2
PIECES = 4


def layer_kernel(scale, n_ctx, n_tp, len_ref, kp_ref, vp_ref, x_hbm, wq_hbm, wk_hbm, wv_hbm, wo_hbm, ks_hbm, vs_hbm, y_ref,
                 x_ref, pool, kv_all, q_ref, new_ref, kbuf, vbuf, o_suf, m_suf, l_suf, flat, att_ref, part, first_in, direct_in, sum_in,
                 x_sem, wsem, ksem, vsem, ring_send, ring_recv, pair_send, pair_recv, send_sem, recv_sem):
    kv_heads, positions, dim = kv_all.shape[2:]
    seqs = x_ref.shape[0]
    model, width = wk_hbm.shape
    inner = wo_hbm.shape[0]
    group = inner // (kv_heads * dim)
    heads = kv_heads * group
    slots = kbuf.shape[2]
    q_blocks = inner // width
    blocks = q_blocks + 2
    bufs = pool.shape[0]
    half = part.shape[2]
    tiles = half // width
    rows = seqs // CHUNKS
    step = seqs // PIECES
    per = PIECES // CHUNKS
    factor = scale * math.log2(math.e)

    here = lax.axis_index('ctx')
    x_right, x_left, x_far = lax.rem(here + 2, n_ctx), lax.rem(here + n_ctx - 2, n_ctx), lax.rem(here + 4, n_ctx)
    partner = here + 1 - 2 * lax.rem(here, 2)
    me = lax.axis_index('tp')
    right, left, far = lax.rem(me + 1, n_tp), lax.rem(me + n_tp - 1, n_tp), lax.rem(me + 2, n_tp)

    def columns(owner, which, size):
        return pl.ds(pl.multiple_of((owner * 2 + which) * half, half), size)

    def fetch_q(j, slot):
        where = pl.ds(pl.multiple_of(j * width, width), width)
        return pltpu.make_async_copy(wq_hbm.at[:, where], pool.at[slot], wsem.at[slot])

    def fetch_o(k, slot):
        away = sum(jnp.where(k == n, ORDER[n][0], 0) for n in range(8))
        which = sum(jnp.where(k == n, ORDER[n][1], 0) for n in range(8))
        start = (lax.rem(me + away, n_tp) * 2 + which) * half
        for t in range(tiles):
            where = pl.ds(pl.multiple_of(start + t * width, width), width)
            pltpu.make_async_copy(wo_hbm.at[:, where], pool.at[slot, pl.ds(t * inner, inner)], wsem.at[slot]).start()

    def weights_here(slot):
        pltpu.make_async_copy(wk_hbm, pool.at[slot], wsem.at[slot]).wait()

    def fetch_suffix(g):
        slot = lax.rem(g, DEPTH)
        which = pl.ds(g * SUB, SUB)
        return (pltpu.make_async_copy(ks_hbm.at[which], kbuf.at[slot], ksem.at[slot]),
                pltpu.make_async_copy(vs_hbm.at[which], vbuf.at[slot], vsem.at[slot]))

    x_copy = pltpu.make_async_copy(x_hbm, x_ref, x_sem)
    x_copy.start()
    for j in range(bufs):
        fetch_q(j, j).start()

    barrier = pltpu.get_barrier_semaphore()
    for axis, peer in (('ctx', x_left), ('ctx', x_right), ('ctx', partner), ('tp', left), ('tp', right)):
        pl.semaphore_signal(barrier, inc=1, device_id={axis: peer}, device_id_type=MESH)

    pick_row = lax.broadcasted_iota(jnp.int32, (positions, positions * kv_heads), 0)
    pick_col = lax.broadcasted_iota(jnp.int32, (positions, positions * kv_heads), 1)
    for kv in range(kv_heads):
        pick = jnp.where(pick_col == pick_row * kv_heads + kv, 1.0, 0.0).astype(BF16)
        for n, ref in enumerate((kp_ref, vp_ref)):
            kv_all[here, n, kv] = jnp.dot(pick, ref[...], preferred_element_type=F32).astype(BF16)
    pl.semaphore_wait(barrier, 5)

    def ring(src, dst, index, peer):
        return pltpu.make_async_remote_copy(src_ref=src, dst_ref=dst, send_sem=ring_send.at[index], recv_sem=ring_recv.at[index], device_id={'ctx': peer}, device_id_type=MESH)

    def pair(slot, index):
        block = kv_all.at[slot]
        return pltpu.make_async_remote_copy(src_ref=block, dst_ref=block, send_sem=pair_send.at[index], recv_sem=pair_recv.at[index], device_id={'ctx': partner}, device_id_type=MESH)

    own = kv_all.at[here]
    ring(own, own, 0, x_right).start()
    ring(own, own, 1, x_left).start()
    pair(here, 0).start()
    x_copy.wait()

    def project_in(j, carry):
        slot = lax.rem(j, bufs)
        weights_here(slot)
        block = jnp.dot(x_ref[...], pool[slot], preferred_element_type=F32).astype(BF16).astype(F32)
        per_block = width // dim

        @pl.when(j < q_blocks)
        def _():
            for i in range(per_block):
                head = j * per_block + i
                q_ref[head // group, pl.ds(lax.rem(head, group), seqs, stride=group), :] = block[:, i * dim:(i + 1) * dim]

        @pl.when(j >= q_blocks)
        def _():
            for i in range(per_block):
                new_ref[j - q_blocks, i] = block[:, i * dim:(i + 1) * dim]

        @pl.when(j + bufs < q_blocks)
        def _():
            fetch_q(j + bufs, slot).start()

        @pl.when(j + bufs == q_blocks)
        def _():
            pltpu.make_async_copy(wk_hbm, pool.at[slot], wsem.at[slot]).start()

        @pl.when(j + bufs == q_blocks + 1)
        def _():
            pltpu.make_async_copy(wv_hbm, pool.at[slot], wsem.at[slot]).start()

        @pl.when(j == 1)
        def _():
            for g in range(min(DEPTH, seqs // SUB)):
                for copy in fetch_suffix(jnp.int32(g)):
                    copy.start()

        @pl.when(j >= blocks - bufs)
        def _():
            fetch_o(j - (blocks - bufs), slot)

        @pl.when(j == blocks - 4)
        def _():
            ring(kv_all.at[x_left], kv_all.at[x_left], 0, x_right).wait_recv()
            ring(kv_all.at[x_left, 0], kv_all.at[x_left, 0], 2, x_right).start()
            ring(kv_all.at[x_right], kv_all.at[x_right], 1, x_left).wait_recv()
            ring(kv_all.at[x_right, 1], kv_all.at[x_right, 1], 3, x_left).start()
            pair(x_left, 1).start()
            pair(x_right, 2).start()

        return carry

    lax.fori_loop(0, blocks, project_in, 0)

    ring(kv_all.at[x_far, 0], kv_all.at[x_far, 0], 2, x_right).wait_recv()
    ring(kv_all.at[x_far, 1], kv_all.at[x_far, 1], 3, x_left).wait_recv()
    pair(x_far, 3).start()

    column = lax.broadcasted_iota(jnp.int32, (heads, slots), 1)
    head_of = lax.broadcasted_iota(jnp.int32, (heads, slots), 0) // group
    place = jnp.where(lax.rem(column, kv_heads) == head_of, column // kv_heads, slots)

    def suffix(g, chunk):
        slot = lax.rem(g, DEPTH)
        for copy in fetch_suffix(g):
            copy.wait()
        base = pl.multiple_of(g * SUB, SUB)
        new = [[new_ref[n, kv, pl.ds(base, SUB)] for kv in range(kv_heads)] for n in range(2)]
        spread = [jnp.concatenate([jnp.broadcast_to(new[n][kv][s:s + 1], (group, dim)) for s in range(SUB) for kv in range(kv_heads)], axis=0) for n in range(2)]
        q_blk = [q_ref[kv, pl.ds(pl.multiple_of(base * group, SUB * group), SUB * group)] for kv in range(kv_heads)]
        q_all = jnp.concatenate([q_blk[kv][s * group:(s + 1) * group] for s in range(SUB) for kv in range(kv_heads)], axis=0)
        q_low = q_all.astype(BF16)
        scores = []
        for s in range(SUB):
            one = lax.dot_general(q_low[s * heads:(s + 1) * heads], kbuf[slot, s], LAST, preferred_element_type=F32)
            scores.append(jnp.where(place < len_ref[base + s], one, -jnp.inf))
        scores = jnp.concatenate(scores, axis=0)
        own_score = jnp.sum(q_all * spread[0], axis=-1, keepdims=True)
        top = jnp.maximum(jnp.max(scores, axis=-1, keepdims=True), own_score)
        e = jnp.exp2((scores - top) * factor)
        e_own = jnp.exp2((own_score - top) * factor)
        total = jnp.sum(e, axis=-1, keepdims=True) + e_own
        e = e.astype(BF16)
        o = [jnp.dot(e[s * heads:(s + 1) * heads], vbuf[slot, s], preferred_element_type=F32) for s in range(SUB)]
        o = jnp.concatenate(o, axis=0) + e_own * spread[1]
        for s in range(SUB):
            for kv in range(kv_heads):
                src = slice(s * heads + kv * group, s * heads + (kv + 1) * group)
                dst = pl.ds(pl.multiple_of((base - chunk * rows + s) * group, group), group)
                o_suf[kv, dst] = o[src]
                m_suf[kv, dst] = top[src]
                l_suf[kv, dst] = total[src]

        @pl.when(g + DEPTH < seqs // SUB)
        def _():
            for copy in fetch_suffix(g + DEPTH):
                copy.start()

    size = min(PREFIX, rows)

    def prefix(n, chunk):
        kv, part_no = lax.rem(n, kv_heads), n // kv_heads
        local = pl.ds(pl.multiple_of(part_no * size * group, size * group), size * group)
        q_low = q_ref[kv, pl.ds(pl.multiple_of((chunk * rows + part_no * size) * group, size * group), size * group)].astype(BF16)
        s = lax.dot_general(q_low, kv_all[:, 0, kv].reshape(n_ctx * positions, dim), LAST, preferred_element_type=F32)
        top_pre = jnp.max(s, axis=-1, keepdims=True)
        e = jnp.exp2((s - top_pre) * factor)
        total_pre = jnp.sum(e, axis=-1, keepdims=True)
        o_pre = jnp.dot(e.astype(BF16), kv_all[:, 1, kv].reshape(n_ctx * positions, dim), preferred_element_type=F32)
        top_suf = m_suf[kv, local]
        top = jnp.maximum(top_pre, top_suf)
        w_pre = jnp.exp2((top_pre - top) * factor)
        w_suf = jnp.exp2((top_suf - top) * factor)
        total = w_pre * total_pre + w_suf * l_suf[kv, local]
        flat[...] = (w_pre * o_pre + w_suf * o_suf[kv, local]) / total
        where = pl.ds(pl.multiple_of(chunk * rows + part_no * size, size), size)
        for h in range(group):
            cols = pl.ds(pl.multiple_of((kv * group + h) * dim, dim), dim)
            att_ref[where, cols] = flat[pl.ds(h, size, stride=group), :].astype(BF16)

    def attend(chunk):
        def body(i, carry):
            suffix(chunk * (rows // SUB) + i, chunk)
            return carry

        lax.fori_loop(0, rows // SUB, body, 0)
        if chunk == 0:
            for index, slot in enumerate((here, x_left, x_right, x_far)):
                other = kv_all.at[slot + partner - here]
                pltpu.make_async_remote_copy(src_ref=other, dst_ref=other, send_sem=pair_send.at[index], recv_sem=pair_recv.at[index], device_id={'ctx': partner}, device_id_type=MESH).wait_recv()

        def body_pre(n, carry):
            prefix(n, chunk)
            return carry

        lax.fori_loop(0, kv_heads * (rows // size), body_pre, 0)

    def copy(kind, way, p, src, dst):
        return pltpu.make_async_remote_copy(src_ref=src, dst_ref=dst, send_sem=send_sem.at[kind, way, p], recv_sem=recv_sem.at[kind, way, p], device_id={'tp': (right, left)[way]}, device_id_type=MESH)

    def span(p):
        return pl.ds(p * step, step)

    started = []

    def launch(*args):
        one = copy(*args)
        one.start()
        started.append(one)

    def mine(chunk):
        return range(chunk * per, (chunk + 1) * per)

    def project_out(chunk, k0, k1):
        which = pl.ds(chunk * rows, rows)

        def body(n, carry):
            k, t = n // tiles, lax.rem(n, tiles)
            slot = lax.rem(k + blocks - bufs, bufs)
            if chunk == 0:
                @pl.when(t == 0)
                def _():
                    weights_here(slot)
            part[k, which, pl.ds(pl.multiple_of(t * width, width), width)] = jnp.dot(att_ref[which, :], pool[slot, pl.ds(pl.multiple_of(t * inner, inner), inner), :], preferred_element_type=F32)
            return carry

        lax.fori_loop(k0 * tiles, k1 * tiles, body, 0)

    def send_parts(chunk):
        project_out(chunk, 0, 1)
        for p in mine(chunk):
            launch(0, 1, p, part.at[0, span(p)], first_in.at[1, span(p)])
        project_out(chunk, 1, 2)
        for p in mine(chunk):
            launch(0, 0, p, part.at[1, span(p)], first_in.at[0, span(p)])
        project_out(chunk, 2, 4)
        for p in mine(chunk):
            launch(1, 0, p, part.at[2, span(p)], direct_in.at[0, span(p)])
            launch(1, 1, p, part.at[3, span(p)], direct_in.at[1, span(p)])
        project_out(chunk, 4, 8)

    def forward_sums(chunk):
        for p in mine(chunk):
            for way, k in ((0, 4), (1, 5)):
                copy(0, way, p, first_in.at[way, span(p)], first_in.at[way, span(p)]).wait_recv()
                part[k, span(p)] += first_in[way, span(p)]
                launch(2, way, p, part.at[k, span(p)], sum_in.at[way, span(p)])

    def finish(chunk):
        for p in mine(chunk):
            for way in (0, 1):
                copy(1, way, p, direct_in.at[way, span(p)], direct_in.at[way, span(p)]).wait_recv()
                copy(2, way, p, sum_in.at[way, span(p)], sum_in.at[way, span(p)]).wait_recv()
            for which in (0, 1):
                total = part[6 + which, span(p)] + sum_in[1 - which, span(p)] + direct_in[which, span(p)]
                total = total + x_ref[span(p), columns(me, which, half)].astype(F32)
                y_ref[span(p), columns(me, which, half)] = total.astype(BF16)
            for way in (0, 1):
                block = y_ref.at[span(p), columns(me, 0, 2 * half)]
                launch(3, way, p, block, block)

    def forward_results(chunk):
        for p in mine(chunk):
            for way, source in ((0, left), (1, right)):
                block = y_ref.at[span(p), columns(source, 0, 2 * half)]
                copy(3, way, p, block, block).wait_recv()
                block = y_ref.at[span(p), columns(source, way, half)]
                launch(4, way, p, block, block)

    for chunk in range(CHUNKS):
        attend(chunk)
        if chunk:
            finish(chunk - 1)
        send_parts(chunk)
        if chunk:
            forward_results(chunk - 1)
        forward_sums(chunk)
    finish(CHUNKS - 1)
    forward_results(CHUNKS - 1)
    for p in range(PIECES):
        for way in (0, 1):
            block = y_ref.at[span(p), columns(far, way, half)]
            copy(4, way, p, block, block).wait_recv()
    for one in started:
        one.wait_send()
    ring(own, own, 0, x_right).wait_send()
    ring(own, own, 1, x_left).wait_send()
    ring(kv_all.at[x_left, 0], kv_all.at[x_left, 0], 2, x_right).wait_send()
    ring(kv_all.at[x_right, 1], kv_all.at[x_right, 1], 3, x_left).wait_send()
    for index, slot in enumerate((here, x_left, x_right, x_far)):
        pair(slot, index).wait_send()


def solution(mesh):
    n_ctx, n_tp = mesh.shape['ctx'], mesh.shape['tp']
    row_axes = ('dp', 'ctx')
    vmem = pl.BlockSpec(memory_space=pltpu.VMEM)
    hbm = pl.BlockSpec(memory_space=pl.ANY)
    dma = pltpu.SemaphoreType.DMA

    def device_step(hidden, w_q, w_k, w_v, w_o, k_prefix, v_prefix, k_suffix, v_suffix, seq_lens):
        seqs, model = hidden.shape
        positions, kv_heads, dim = k_prefix.shape
        slots = k_suffix.shape[1] * kv_heads
        inner = w_q.shape[1]
        group = inner // (kv_heads * dim)
        width = w_k.shape[1]
        half = model // (2 * n_tp)
        rows = seqs // CHUNKS
        size = min(PREFIX, rows)
        return pl.pallas_call(
            functools.partial(layer_kernel, dim ** -0.5, n_ctx, n_tp),
            name='layer',
            out_shape=jax.ShapeDtypeStruct((seqs, model), BF16),
            in_specs=[pl.BlockSpec(memory_space=pltpu.SMEM), vmem, vmem] + [hbm] * 7,
            out_specs=vmem,
            scratch_shapes=[
                pltpu.VMEM((seqs, model), BF16),
                pltpu.VMEM((8, model, width), BF16),
                pltpu.VMEM((n_ctx, 2, kv_heads, positions, dim), BF16),
                pltpu.VMEM((kv_heads, seqs * group, dim), F32),
                pltpu.VMEM((2, kv_heads, seqs, dim), F32),
                pltpu.VMEM((DEPTH, SUB, slots, dim), BF16),
                pltpu.VMEM((DEPTH, SUB, slots, dim), BF16),
                pltpu.VMEM((kv_heads, rows * group, dim), F32),
                pltpu.VMEM((kv_heads, rows * group, 1), F32),
                pltpu.VMEM((kv_heads, rows * group, 1), F32),
                pltpu.VMEM((size * group, dim), F32),
                pltpu.VMEM((seqs, inner), BF16),
                pltpu.VMEM((8, seqs, half), F32),
                pltpu.VMEM((2, seqs, half), F32),
                pltpu.VMEM((2, seqs, half), F32),
                pltpu.VMEM((2, seqs, half), F32),
                dma, dma((8,)), dma((DEPTH,)), dma((DEPTH,)), dma((4,)), dma((4,)), dma((4,)), dma((4,)), dma((5, 2, PIECES)), dma((5, 2, PIECES)),
            ],
            compiler_params=pltpu.CompilerParams(collective_id=0, has_side_effects=True, vmem_limit_bytes=67000000),
        )(seq_lens, k_prefix.reshape(positions * kv_heads, dim), v_prefix.reshape(positions * kv_heads, dim), hidden, w_q, w_k, w_v, w_o, k_suffix.reshape(seqs, slots, dim), v_suffix.reshape(seqs, slots, dim))

    spec_in = (P(row_axes, None), P(None, 'tp'), P(None, 'tp'), P(None, 'tp'), P('tp', None), P(row_axes, 'tp', None), P(row_axes, 'tp', None), P(row_axes, None, 'tp', None), P(row_axes, None, 'tp', None), P(row_axes))
    return jax.shard_map(device_step, mesh=mesh, in_specs=spec_in, out_specs=P(row_axes, None), check_vma=False)
```

```python
import functools
import math

import jax
import jax.numpy as jnp
from jax import lax
from jax.experimental import pallas as pl
from jax.experimental.pallas import tpu as pltpu
from jax.sharding import PartitionSpec as P

MESH = pl.DeviceIdType.MESH
F32, BF16 = jnp.float32, jnp.bfloat16
LAST = (((1,), (1,)), ((), ()))

ORDER = ((2, 0), (2, 1), (1, 0), (3, 1), (1, 1), (3, 0), (0, 0), (0, 1))
SUB = 8
EARLY = 2
DEPTH = 4
PREFIX = 32
CHUNKS = 4
PIECES = 8


def layer_kernel(scale, n_ctx, n_tp, len_ref, kp_ref, vp_ref, x_hbm, wq_hbm, wk_hbm, wv_hbm, wo_hbm, ks_hbm, vs_hbm, y_hbm,
                 y_ref, x_ref, pool, kv_all, q_ref, new_ref, kbuf, vbuf, o_suf, m_suf, l_suf, flat, att_ref, part, first_in, direct_in, sum_in,
                 x_sem, y_sem, wsem, ksem, vsem, ring_send, ring_recv, pair_send, pair_recv, send_sem, recv_sem):
    kv_heads, positions, dim = kv_all.shape[2:]
    seqs = x_ref.shape[0]
    model, width = wk_hbm.shape
    inner = wo_hbm.shape[0]
    group = inner // (kv_heads * dim)
    heads = kv_heads * group
    slots = kbuf.shape[2]
    q_blocks = inner // width
    blocks = q_blocks + 2
    bufs = pool.shape[0]
    half = part.shape[2]
    tiles = half // width
    rows = seqs // CHUNKS
    step = seqs // PIECES
    per = PIECES // CHUNKS
    factor = scale * math.log2(math.e)

    here = lax.axis_index('ctx')
    x_right, x_left, x_far = lax.rem(here + 2, n_ctx), lax.rem(here + n_ctx - 2, n_ctx), lax.rem(here + 4, n_ctx)
    partner = here + 1 - 2 * lax.rem(here, 2)
    me = lax.axis_index('tp')
    right, left, far = lax.rem(me + 1, n_tp), lax.rem(me + n_tp - 1, n_tp), lax.rem(me + 2, n_tp)

    def columns(owner, which, size):
        return pl.ds(pl.multiple_of((owner * 2 + which) * half, half), size)

    def fetch_q(j, slot):
        where = pl.ds(pl.multiple_of(j * width, width), width)
        return pltpu.make_async_copy(wq_hbm.at[:, where], pool.at[slot], wsem.at[slot])

    def fetch_o(k, slot):
        away = sum(jnp.where(k == n, ORDER[n][0], 0) for n in range(8))
        which = sum(jnp.where(k == n, ORDER[n][1], 0) for n in range(8))
        start = (lax.rem(me + away, n_tp) * 2 + which) * half
        for t in range(tiles):
            where = pl.ds(pl.multiple_of(start + t * width, width), width)
            pltpu.make_async_copy(wo_hbm.at[:, where], pool.at[slot, pl.ds(t * inner, inner)], wsem.at[slot]).start()

    def weights_here(slot):
        pltpu.make_async_copy(wk_hbm, pool.at[slot], wsem.at[slot]).wait()

    def fetch_suffix(g):
        slot = lax.rem(g, DEPTH)
        which = pl.ds(g * SUB, SUB)
        return (pltpu.make_async_copy(ks_hbm.at[which], kbuf.at[slot], ksem.at[slot]),
                pltpu.make_async_copy(vs_hbm.at[which], vbuf.at[slot], vsem.at[slot]))

    x_copy = pltpu.make_async_copy(x_hbm, x_ref, x_sem)
    x_copy.start()
    for j in range(bufs):
        fetch_q(j, j).start()

    barrier = pltpu.get_barrier_semaphore()
    for axis, peer in (('ctx', x_left), ('ctx', x_right), ('ctx', partner), ('tp', left), ('tp', right)):
        pl.semaphore_signal(barrier, inc=1, device_id={axis: peer}, device_id_type=MESH)

    pick_row = lax.broadcasted_iota(jnp.int32, (positions, positions * kv_heads), 0)
    pick_col = lax.broadcasted_iota(jnp.int32, (positions, positions * kv_heads), 1)
    for kv in range(kv_heads):
        pick = jnp.where(pick_col == pick_row * kv_heads + kv, 1.0, 0.0).astype(BF16)
        for n, ref in enumerate((kp_ref, vp_ref)):
            kv_all[here, n, kv] = jnp.dot(pick, ref[...], preferred_element_type=F32).astype(BF16)
    pl.semaphore_wait(barrier, 5)

    def ring(src, dst, index, peer):
        return pltpu.make_async_remote_copy(src_ref=src, dst_ref=dst, send_sem=ring_send.at[index], recv_sem=ring_recv.at[index], device_id={'ctx': peer}, device_id_type=MESH)

    def pair(slot, index):
        block = kv_all.at[slot]
        return pltpu.make_async_remote_copy(src_ref=block, dst_ref=block, send_sem=pair_send.at[index], recv_sem=pair_recv.at[index], device_id={'ctx': partner}, device_id_type=MESH)

    own = kv_all.at[here]
    ring(own, own, 0, x_right).start()
    ring(own, own, 1, x_left).start()
    pair(here, 0).start()
    x_copy.wait()

    def project_in(j, carry):
        slot = lax.rem(j, bufs)
        weights_here(slot)
        block = jnp.dot(x_ref[...], pool[slot], preferred_element_type=F32).astype(BF16).astype(F32)
        per_block = width // dim

        @pl.when(j < q_blocks)
        def _():
            for i in range(per_block):
                head = j * per_block + i
                q_ref[head // group, pl.ds(lax.rem(head, group), seqs, stride=group), :] = block[:, i * dim:(i + 1) * dim]

        @pl.when(j >= q_blocks)
        def _():
            for i in range(per_block):
                new_ref[j - q_blocks, i] = block[:, i * dim:(i + 1) * dim]

        @pl.when(j + bufs < q_blocks)
        def _():
            fetch_q(j + bufs, slot).start()

        @pl.when(j + bufs == q_blocks)
        def _():
            pltpu.make_async_copy(wk_hbm, pool.at[slot], wsem.at[slot]).start()

        @pl.when(j + bufs == q_blocks + 1)
        def _():
            pltpu.make_async_copy(wv_hbm, pool.at[slot], wsem.at[slot]).start()

        @pl.when(j == 1)
        def _():
            for g in range(min(DEPTH, seqs // SUB)):
                for copy in fetch_suffix(jnp.int32(g)):
                    copy.start()

        @pl.when((j >= blocks - bufs) & (j < blocks - bufs + EARLY))
        def _():
            fetch_o(j - (blocks - bufs), slot)

        @pl.when(j == blocks - 4)
        def _():
            ring(kv_all.at[x_left], kv_all.at[x_left], 0, x_right).wait_recv()
            ring(kv_all.at[x_left, 0], kv_all.at[x_left, 0], 2, x_right).start()
            ring(kv_all.at[x_right], kv_all.at[x_right], 1, x_left).wait_recv()
            ring(kv_all.at[x_right, 1], kv_all.at[x_right, 1], 3, x_left).start()
            pair(x_left, 1).start()
            pair(x_right, 2).start()

        return carry

    lax.fori_loop(0, blocks, project_in, 0)

    ring(kv_all.at[x_far, 0], kv_all.at[x_far, 0], 2, x_right).wait_recv()
    ring(kv_all.at[x_far, 1], kv_all.at[x_far, 1], 3, x_left).wait_recv()
    pair(x_far, 3).start()

    column = lax.broadcasted_iota(jnp.int32, (heads, slots), 1)
    head_of = lax.broadcasted_iota(jnp.int32, (heads, slots), 0) // group
    place = jnp.where(lax.rem(column, kv_heads) == head_of, column // kv_heads, slots)

    def suffix(g, chunk):
        slot = lax.rem(g, DEPTH)
        for copy in fetch_suffix(g):
            copy.wait()
        base = pl.multiple_of(g * SUB, SUB)
        new = [[new_ref[n, kv, pl.ds(base, SUB)] for kv in range(kv_heads)] for n in range(2)]
        spread = [jnp.concatenate([jnp.broadcast_to(new[n][kv][s:s + 1], (group, dim)) for s in range(SUB) for kv in range(kv_heads)], axis=0) for n in range(2)]
        q_blk = [q_ref[kv, pl.ds(pl.multiple_of(base * group, SUB * group), SUB * group)] for kv in range(kv_heads)]
        q_all = jnp.concatenate([q_blk[kv][s * group:(s + 1) * group] for s in range(SUB) for kv in range(kv_heads)], axis=0)
        q_low = q_all.astype(BF16)
        scores = []
        for s in range(SUB):
            one = lax.dot_general(q_low[s * heads:(s + 1) * heads], kbuf[slot, s], LAST, preferred_element_type=F32)
            scores.append(jnp.where(place < len_ref[base + s], one, -jnp.inf))
        scores = jnp.concatenate(scores, axis=0)
        own_score = jnp.sum(q_all * spread[0], axis=-1, keepdims=True)
        top = jnp.maximum(jnp.max(scores, axis=-1, keepdims=True), own_score)
        e = jnp.exp2((scores - top) * factor)
        e_own = jnp.exp2((own_score - top) * factor)
        total = jnp.sum(e, axis=-1, keepdims=True) + e_own
        e = e.astype(BF16)
        o = [jnp.dot(e[s * heads:(s + 1) * heads], vbuf[slot, s], preferred_element_type=F32) for s in range(SUB)]
        o = jnp.concatenate(o, axis=0) + e_own * spread[1]
        for s in range(SUB):
            for kv in range(kv_heads):
                src = slice(s * heads + kv * group, s * heads + (kv + 1) * group)
                dst = pl.ds(pl.multiple_of((base - chunk * rows + s) * group, group), group)
                o_suf[kv, dst] = o[src]
                m_suf[kv, dst] = top[src]
                l_suf[kv, dst] = total[src]

        @pl.when(g + DEPTH < seqs // SUB)
        def _():
            for copy in fetch_suffix(g + DEPTH):
                copy.start()

        share = -(-(8 - EARLY) // (rows // SUB))
        for i in range(share):
            k = EARLY + g * share + i

            @pl.when((g < rows // SUB) & (k < 8))
            def _():
                fetch_o(k, lax.rem(k + blocks - bufs, bufs))

    size = min(PREFIX, rows)

    def prefix(n, chunk):
        kv, part_no = lax.rem(n, kv_heads), n // kv_heads
        local = pl.ds(pl.multiple_of(part_no * size * group, size * group), size * group)
        q_low = q_ref[kv, pl.ds(pl.multiple_of((chunk * rows + part_no * size) * group, size * group), size * group)].astype(BF16)
        s = lax.dot_general(q_low, kv_all[:, 0, kv].reshape(n_ctx * positions, dim), LAST, preferred_element_type=F32)
        top_pre = jnp.max(s, axis=-1, keepdims=True)
        e = jnp.exp2((s - top_pre) * factor)
        total_pre = jnp.sum(e, axis=-1, keepdims=True)
        o_pre = jnp.dot(e.astype(BF16), kv_all[:, 1, kv].reshape(n_ctx * positions, dim), preferred_element_type=F32)
        top_suf = m_suf[kv, local]
        top = jnp.maximum(top_pre, top_suf)
        w_pre = jnp.exp2((top_pre - top) * factor)
        w_suf = jnp.exp2((top_suf - top) * factor)
        total = w_pre * total_pre + w_suf * l_suf[kv, local]
        flat[...] = (w_pre * o_pre + w_suf * o_suf[kv, local]) / total
        where = pl.ds(pl.multiple_of(chunk * rows + part_no * size, size), size)
        for h in range(group):
            cols = pl.ds(pl.multiple_of((kv * group + h) * dim, dim), dim)
            att_ref[where, cols] = flat[pl.ds(h, size, stride=group), :].astype(BF16)

    def attend(chunk):
        def body(i, carry):
            suffix(chunk * (rows // SUB) + i, chunk)
            return carry

        lax.fori_loop(0, rows // SUB, body, 0)

        @pl.when(chunk == 0)
        def _():
            for index, slot in enumerate((here, x_left, x_right, x_far)):
                other = kv_all.at[slot + partner - here]
                pltpu.make_async_remote_copy(src_ref=other, dst_ref=other, send_sem=pair_send.at[index], recv_sem=pair_recv.at[index], device_id={'ctx': partner}, device_id_type=MESH).wait_recv()

        def body_pre(n, carry):
            prefix(n, chunk)
            return carry

        lax.fori_loop(0, kv_heads * (rows // size), body_pre, 0)

    def copy(kind, way, p, src, dst):
        return pltpu.make_async_remote_copy(src_ref=src, dst_ref=dst, send_sem=send_sem.at[kind, way, p], recv_sem=recv_sem.at[kind, way, p], device_id={'tp': (right, left)[way]}, device_id_type=MESH)

    def here_only(kind, way, p, ref):
        return copy(kind, way, p, ref, ref)

    def span(p):
        return pl.ds(pl.multiple_of(p * step, step), step)

    def pieces_of(chunk, action):
        def body(p, carry):
            action(p)
            return carry

        lax.fori_loop(chunk * per, (chunk + 1) * per, body, 0)

    def first(way, p):
        return copy(0, way, p, part.at[1 - way, span(p)], first_in.at[way, span(p)])

    def direct(way, p):
        return copy(1, way, p, part.at[2 + way, span(p)], direct_in.at[way, span(p)])

    def summed(way, p):
        return copy(2, way, p, part.at[4 + way, span(p)], sum_in.at[way, span(p)])

    def result(way, p, owner):
        return here_only(3, way, p, y_ref.at[span(p), columns(owner, 0, 2 * half)])

    def passed_on(way, p, owner):
        return here_only(4, way, p, y_ref.at[span(p), columns(owner, way, half)])

    def project_out(chunk, k0, k1):
        which = pl.ds(pl.multiple_of(chunk * rows, rows), rows)

        def body(n, carry):
            k, t = n // tiles, lax.rem(n, tiles)
            slot = lax.rem(k + blocks - bufs, bufs)

            @pl.when((chunk == 0) & (t == 0))
            def _():
                weights_here(slot)

            part[k, which, pl.ds(pl.multiple_of(t * width, width), width)] = jnp.dot(att_ref[which, :], pool[slot, pl.ds(pl.multiple_of(t * inner, inner), inner), :], preferred_element_type=F32)
            return carry

        lax.fori_loop(k0 * tiles, k1 * tiles, body, 0)

    def send_parts(chunk):
        def go(k, carry):
            project_out(chunk, k, k + 1)

            @pl.when(k == 0)
            def _():
                pieces_of(chunk, lambda p: first(1, p).start())

            @pl.when(k == 1)
            def _():
                pieces_of(chunk, lambda p: first(0, p).start())

            @pl.when(k == 3)
            def _():
                def both(p):
                    direct(0, p).start()
                    direct(1, p).start()

                pieces_of(chunk, both)

            return carry

        lax.fori_loop(0, 8, go, 0)

    def forward_sums(chunk):
        def action(p):
            for way in (0, 1):
                first(way, p).wait_recv()
                part[4 + way, span(p)] += first_in[way, span(p)]
                summed(way, p).start()

        pieces_of(chunk, action)

    def finish(chunk):
        def action(p):
            for way in (0, 1):
                direct(way, p).wait_recv()
                summed(way, p).wait_recv()
            for which in (0, 1):
                total = part[6 + which, span(p)] + sum_in[1 - which, span(p)] + direct_in[which, span(p)]
                total = total + x_ref[span(p), columns(me, which, half)].astype(F32)
                y_ref[span(p), columns(me, which, half)] = total.astype(BF16)
            for way in (0, 1):
                result(way, p, me).start()

        pieces_of(chunk, action)

    def forward_results(chunk):
        def action(p):
            for way, source in ((0, left), (1, right)):
                result(way, p, source).wait_recv()
                passed_on(way, p, source).start()

        pieces_of(chunk, action)

    def pipeline(stage, carry):
        @pl.when(stage < CHUNKS)
        def _():
            attend(stage)

        @pl.when((stage >= 1) & (stage <= CHUNKS))
        def _():
            forward_sums(stage - 1)

        @pl.when((stage >= 2) & (stage <= CHUNKS + 1))
        def _():
            finish(stage - 2)

        @pl.when(stage < CHUNKS)
        def _():
            send_parts(stage)

        @pl.when(stage >= 3)
        def _():
            forward_results(stage - 3)

        return carry

    lax.fori_loop(0, CHUNKS + 3, pipeline, 0)

    def last(p, carry):
        for way in (0, 1):
            passed_on(way, p, far).wait_recv()
        pltpu.make_async_copy(y_ref.at[span(p)], y_hbm.at[span(p)], y_sem).start()
        return carry

    lax.fori_loop(0, PIECES, last, 0)

    def sent(p, carry):
        for way, source in ((0, left), (1, right)):
            first(way, p).wait_send()
            direct(way, p).wait_send()
            summed(way, p).wait_send()
            result(way, p, me).wait_send()
            passed_on(way, p, source).wait_send()
        return carry

    lax.fori_loop(0, PIECES, sent, 0)
    ring(own, own, 0, x_right).wait_send()
    ring(own, own, 1, x_left).wait_send()
    ring(kv_all.at[x_left, 0], kv_all.at[x_left, 0], 2, x_right).wait_send()
    ring(kv_all.at[x_right, 1], kv_all.at[x_right, 1], 3, x_left).wait_send()
    for index, slot in enumerate((here, x_left, x_right, x_far)):
        pair(slot, index).wait_send()
    pltpu.make_async_copy(y_ref, y_hbm, y_sem).wait()


def solution(mesh):
    n_ctx, n_tp = mesh.shape['ctx'], mesh.shape['tp']
    row_axes = ('dp', 'ctx')
    vmem = pl.BlockSpec(memory_space=pltpu.VMEM)
    hbm = pl.BlockSpec(memory_space=pl.ANY)
    dma = pltpu.SemaphoreType.DMA

    def device_step(hidden, w_q, w_k, w_v, w_o, k_prefix, v_prefix, k_suffix, v_suffix, seq_lens):
        seqs, model = hidden.shape
        positions, kv_heads, dim = k_prefix.shape
        slots = k_suffix.shape[1] * kv_heads
        inner = w_q.shape[1]
        group = inner // (kv_heads * dim)
        width = w_k.shape[1]
        half = model // (2 * n_tp)
        rows = seqs // CHUNKS
        size = min(PREFIX, rows)
        return pl.pallas_call(
            functools.partial(layer_kernel, dim ** -0.5, n_ctx, n_tp),
            name='layer',
            out_shape=jax.ShapeDtypeStruct((seqs, model), BF16),
            in_specs=[pl.BlockSpec(memory_space=pltpu.SMEM), vmem, vmem] + [hbm] * 7,
            out_specs=hbm,
            scratch_shapes=[
                pltpu.VMEM((seqs, model), BF16),
                pltpu.VMEM((seqs, model), BF16),
                pltpu.VMEM((8, model, width), BF16),
                pltpu.VMEM((n_ctx, 2, kv_heads, positions, dim), BF16),
                pltpu.VMEM((kv_heads, seqs * group, dim), F32),
                pltpu.VMEM((2, kv_heads, seqs, dim), F32),
                pltpu.VMEM((DEPTH, SUB, slots, dim), BF16),
                pltpu.VMEM((DEPTH, SUB, slots, dim), BF16),
                pltpu.VMEM((kv_heads, rows * group, dim), F32),
                pltpu.VMEM((kv_heads, rows * group, 1), F32),
                pltpu.VMEM((kv_heads, rows * group, 1), F32),
                pltpu.VMEM((size * group, dim), F32),
                pltpu.VMEM((seqs, inner), BF16),
                pltpu.VMEM((8, seqs, half), F32),
                pltpu.VMEM((2, seqs, half), F32),
                pltpu.VMEM((2, seqs, half), F32),
                pltpu.VMEM((2, seqs, half), F32),
                dma, dma, dma((8,)), dma((DEPTH,)), dma((DEPTH,)), dma((4,)), dma((4,)), dma((4,)), dma((4,)), dma((5, 2, PIECES)), dma((5, 2, PIECES)),
            ],
            compiler_params=pltpu.CompilerParams(collective_id=0, has_side_effects=True, vmem_limit_bytes=67000000),
        )(seq_lens, k_prefix.reshape(positions * kv_heads, dim), v_prefix.reshape(positions * kv_heads, dim), hidden, w_q, w_k, w_v, w_o, k_suffix.reshape(seqs, slots, dim), v_suffix.reshape(seqs, slots, dim))

    spec_in = (P(row_axes, None), P(None, 'tp'), P(None, 'tp'), P(None, 'tp'), P('tp', None), P(row_axes, 'tp', None), P(row_axes, 'tp', None), P(row_axes, None, 'tp', None), P(row_axes, None, 'tp', None), P(row_axes))
    return jax.shard_map(device_step, mesh=mesh, in_specs=spec_in, out_specs=P(row_axes, None), check_vma=False)
```

```python
import functools
import math

import jax
import jax.numpy as jnp
from jax import lax
from jax.experimental import pallas as pl
from jax.experimental.pallas import tpu as pltpu
from jax.sharding import PartitionSpec as P

MESH = pl.DeviceIdType.MESH
F32, BF16 = jnp.float32, jnp.bfloat16
LAST = (((1,), (1,)), ((), ()))

ORDER = ((2, 0), (2, 1), (1, 0), (3, 1), (1, 1), (3, 0), (0, 0), (0, 1))
SUB = 8
EARLY = 2
DEPTH = 4
PREFIX = 32
CHUNKS = 2
PIECES = 8


def layer_kernel(scale, n_ctx, n_tp, len_ref, kp_ref, vp_ref, x_hbm, wq_hbm, wk_hbm, wv_hbm, wo_hbm, ks_hbm, vs_hbm, y_hbm,
                 y_ref, x_ref, pool, kv_all, q_ref, new_ref, kbuf, vbuf, o_suf, m_suf, l_suf, flat, att_ref, part, first_in, direct_in, sum_in,
                 x_sem, y_sem, wsem, ksem, vsem, ring_send, ring_recv, pair_send, pair_recv, send_sem, recv_sem):
    kv_heads, positions, dim = kv_all.shape[2:]
    seqs = x_ref.shape[0]
    model, width = wk_hbm.shape
    inner = wo_hbm.shape[0]
    group = inner // (kv_heads * dim)
    heads = kv_heads * group
    slots = kbuf.shape[2]
    q_blocks = inner // width
    blocks = q_blocks + 2
    bufs = pool.shape[0]
    half = part.shape[2]
    tiles = half // width
    rows = seqs // CHUNKS
    step = seqs // PIECES
    per = PIECES // CHUNKS
    factor = scale * math.log2(math.e)

    here = lax.axis_index('ctx')
    x_right, x_left, x_far = lax.rem(here + 2, n_ctx), lax.rem(here + n_ctx - 2, n_ctx), lax.rem(here + 4, n_ctx)
    partner = here + 1 - 2 * lax.rem(here, 2)
    me = lax.axis_index('tp')
    right, left, far = lax.rem(me + 1, n_tp), lax.rem(me + n_tp - 1, n_tp), lax.rem(me + 2, n_tp)

    def columns(owner, which, size):
        return pl.ds(pl.multiple_of((owner * 2 + which) * half, half), size)

    def fetch_q(j, slot):
        where = pl.ds(pl.multiple_of(j * width, width), width)
        return pltpu.make_async_copy(wq_hbm.at[:, where], pool.at[slot], wsem.at[slot])

    def fetch_o(k, slot):
        away = sum(jnp.where(k == n, ORDER[n][0], 0) for n in range(8))
        which = sum(jnp.where(k == n, ORDER[n][1], 0) for n in range(8))
        start = (lax.rem(me + away, n_tp) * 2 + which) * half
        for t in range(tiles):
            where = pl.ds(pl.multiple_of(start + t * width, width), width)
            pltpu.make_async_copy(wo_hbm.at[:, where], pool.at[slot, pl.ds(t * inner, inner)], wsem.at[slot]).start()

    def weights_here(slot):
        pltpu.make_async_copy(wk_hbm, pool.at[slot], wsem.at[slot]).wait()

    def fetch_suffix(g):
        slot = lax.rem(g, DEPTH)
        which = pl.ds(g * SUB, SUB)
        return (pltpu.make_async_copy(ks_hbm.at[which], kbuf.at[slot], ksem.at[slot]),
                pltpu.make_async_copy(vs_hbm.at[which], vbuf.at[slot], vsem.at[slot]))

    x_copy = pltpu.make_async_copy(x_hbm, x_ref, x_sem)
    x_copy.start()
    for j in range(bufs):
        fetch_q(j, j).start()

    barrier = pltpu.get_barrier_semaphore()
    for axis, peer in (('ctx', x_left), ('ctx', x_right), ('ctx', partner), ('tp', left), ('tp', right)):
        pl.semaphore_signal(barrier, inc=1, device_id={axis: peer}, device_id_type=MESH)

    pick_row = lax.broadcasted_iota(jnp.int32, (positions, positions * kv_heads), 0)
    pick_col = lax.broadcasted_iota(jnp.int32, (positions, positions * kv_heads), 1)
    for kv in range(kv_heads):
        pick = jnp.where(pick_col == pick_row * kv_heads + kv, 1.0, 0.0).astype(BF16)
        for n, ref in enumerate((kp_ref, vp_ref)):
            kv_all[here, n, kv] = jnp.dot(pick, ref[...], preferred_element_type=F32).astype(BF16)
    pl.semaphore_wait(barrier, 5)

    def ring(src, dst, index, peer):
        return pltpu.make_async_remote_copy(src_ref=src, dst_ref=dst, send_sem=ring_send.at[index], recv_sem=ring_recv.at[index], device_id={'ctx': peer}, device_id_type=MESH)

    def pair(slot, index):
        block = kv_all.at[slot]
        return pltpu.make_async_remote_copy(src_ref=block, dst_ref=block, send_sem=pair_send.at[index], recv_sem=pair_recv.at[index], device_id={'ctx': partner}, device_id_type=MESH)

    own = kv_all.at[here]
    ring(own, own, 0, x_right).start()
    ring(own, own, 1, x_left).start()
    pair(here, 0).start()
    x_copy.wait()

    def project_in(j, carry):
        slot = lax.rem(j, bufs)
        weights_here(slot)
        block = jnp.dot(x_ref[...], pool[slot], preferred_element_type=F32).astype(BF16).astype(F32)
        per_block = width // dim

        @pl.when(j < q_blocks)
        def _():
            for i in range(per_block):
                head = j * per_block + i
                q_ref[head // group, pl.ds(lax.rem(head, group), seqs, stride=group), :] = block[:, i * dim:(i + 1) * dim]

        @pl.when(j >= q_blocks)
        def _():
            for i in range(per_block):
                new_ref[j - q_blocks, i] = block[:, i * dim:(i + 1) * dim]

        @pl.when(j + bufs < q_blocks)
        def _():
            fetch_q(j + bufs, slot).start()

        @pl.when(j + bufs == q_blocks)
        def _():
            pltpu.make_async_copy(wk_hbm, pool.at[slot], wsem.at[slot]).start()

        @pl.when(j + bufs == q_blocks + 1)
        def _():
            pltpu.make_async_copy(wv_hbm, pool.at[slot], wsem.at[slot]).start()

        @pl.when(j == 1)
        def _():
            for g in range(min(DEPTH, seqs // SUB)):
                for copy in fetch_suffix(jnp.int32(g)):
                    copy.start()

        @pl.when((j >= blocks - bufs) & (j < blocks - bufs + EARLY))
        def _():
            fetch_o(j - (blocks - bufs), slot)

        @pl.when(j == blocks - 4)
        def _():
            ring(kv_all.at[x_left], kv_all.at[x_left], 0, x_right).wait_recv()
            ring(kv_all.at[x_left, 0], kv_all.at[x_left, 0], 2, x_right).start()
            ring(kv_all.at[x_right], kv_all.at[x_right], 1, x_left).wait_recv()
            ring(kv_all.at[x_right, 1], kv_all.at[x_right, 1], 3, x_left).start()
            pair(x_left, 1).start()
            pair(x_right, 2).start()

        return carry

    lax.fori_loop(0, blocks, project_in, 0)

    ring(kv_all.at[x_far, 0], kv_all.at[x_far, 0], 2, x_right).wait_recv()
    ring(kv_all.at[x_far, 1], kv_all.at[x_far, 1], 3, x_left).wait_recv()
    pair(x_far, 3).start()

    column = lax.broadcasted_iota(jnp.int32, (heads, slots), 1)
    head_of = lax.broadcasted_iota(jnp.int32, (heads, slots), 0) // group
    place = jnp.where(lax.rem(column, kv_heads) == head_of, column // kv_heads, slots)

    def suffix(g, chunk):
        slot = lax.rem(g, DEPTH)
        for copy in fetch_suffix(g):
            copy.wait()
        base = pl.multiple_of(g * SUB, SUB)
        new = [[new_ref[n, kv, pl.ds(base, SUB)] for kv in range(kv_heads)] for n in range(2)]
        spread = [jnp.concatenate([jnp.broadcast_to(new[n][kv][s:s + 1], (group, dim)) for s in range(SUB) for kv in range(kv_heads)], axis=0) for n in range(2)]
        q_blk = [q_ref[kv, pl.ds(pl.multiple_of(base * group, SUB * group), SUB * group)] for kv in range(kv_heads)]
        q_all = jnp.concatenate([q_blk[kv][s * group:(s + 1) * group] for s in range(SUB) for kv in range(kv_heads)], axis=0)
        q_low = q_all.astype(BF16)
        scores = []
        for s in range(SUB):
            one = lax.dot_general(q_low[s * heads:(s + 1) * heads], kbuf[slot, s], LAST, preferred_element_type=F32)
            scores.append(jnp.where(place < len_ref[base + s], one, -jnp.inf))
        scores = jnp.concatenate(scores, axis=0)
        own_score = jnp.sum(q_all * spread[0], axis=-1, keepdims=True)
        top = jnp.maximum(jnp.max(scores, axis=-1, keepdims=True), own_score)
        e = jnp.exp2((scores - top) * factor)
        e_own = jnp.exp2((own_score - top) * factor)
        total = jnp.sum(e, axis=-1, keepdims=True) + e_own
        e = e.astype(BF16)
        o = [jnp.dot(e[s * heads:(s + 1) * heads], vbuf[slot, s], preferred_element_type=F32) for s in range(SUB)]
        o = jnp.concatenate(o, axis=0) + e_own * spread[1]
        for s in range(SUB):
            for kv in range(kv_heads):
                src = slice(s * heads + kv * group, s * heads + (kv + 1) * group)
                dst = pl.ds(pl.multiple_of((base - chunk * rows + s) * group, group), group)
                o_suf[kv, dst] = o[src]
                m_suf[kv, dst] = top[src]
                l_suf[kv, dst] = total[src]

        @pl.when(g + DEPTH < seqs // SUB)
        def _():
            for copy in fetch_suffix(g + DEPTH):
                copy.start()

        begin = max(0, rows // SUB - 4)
        share = -(-(8 - EARLY) // (rows // SUB - begin))
        for i in range(share):
            k = EARLY + (g - begin) * share + i

            @pl.when((g >= begin) & (g < rows // SUB) & (k < 8))
            def _():
                fetch_o(k, lax.rem(k + blocks - bufs, bufs))

    size = min(PREFIX, rows)

    def prefix(n, chunk):
        kv, part_no = lax.rem(n, kv_heads), n // kv_heads
        local = pl.ds(pl.multiple_of(part_no * size * group, size * group), size * group)
        q_low = q_ref[kv, pl.ds(pl.multiple_of((chunk * rows + part_no * size) * group, size * group), size * group)].astype(BF16)
        s = lax.dot_general(q_low, kv_all[:, 0, kv].reshape(n_ctx * positions, dim), LAST, preferred_element_type=F32)
        top_pre = jnp.max(s, axis=-1, keepdims=True)
        e = jnp.exp2((s - top_pre) * factor)
        total_pre = jnp.sum(e, axis=-1, keepdims=True)
        o_pre = jnp.dot(e.astype(BF16), kv_all[:, 1, kv].reshape(n_ctx * positions, dim), preferred_element_type=F32)
        top_suf = m_suf[kv, local]
        top = jnp.maximum(top_pre, top_suf)
        w_pre = jnp.exp2((top_pre - top) * factor)
        w_suf = jnp.exp2((top_suf - top) * factor)
        total = w_pre * total_pre + w_suf * l_suf[kv, local]
        flat[...] = (w_pre * o_pre + w_suf * o_suf[kv, local]) / total
        where = pl.ds(pl.multiple_of(chunk * rows + part_no * size, size), size)
        for h in range(group):
            cols = pl.ds(pl.multiple_of((kv * group + h) * dim, dim), dim)
            att_ref[where, cols] = flat[pl.ds(h, size, stride=group), :].astype(BF16)

    def attend(chunk):
        def body(i, carry):
            suffix(chunk * (rows // SUB) + i, chunk)
            return carry

        lax.fori_loop(0, rows // SUB, body, 0)

        @pl.when(chunk == 0)
        def _():
            for index, slot in enumerate((here, x_left, x_right, x_far)):
                other = kv_all.at[slot + partner - here]
                pltpu.make_async_remote_copy(src_ref=other, dst_ref=other, send_sem=pair_send.at[index], recv_sem=pair_recv.at[index], device_id={'ctx': partner}, device_id_type=MESH).wait_recv()

        def body_pre(n, carry):
            prefix(n, chunk)
            return carry

        lax.fori_loop(0, kv_heads * (rows // size), body_pre, 0)

    def copy(kind, way, p, src, dst):
        return pltpu.make_async_remote_copy(src_ref=src, dst_ref=dst, send_sem=send_sem.at[kind, way, p], recv_sem=recv_sem.at[kind, way, p], device_id={'tp': (right, left)[way]}, device_id_type=MESH)

    def here_only(kind, way, p, ref):
        return copy(kind, way, p, ref, ref)

    def span(p):
        return pl.ds(pl.multiple_of(p * step, step), step)

    def pieces_of(chunk, action):
        def body(p, carry):
            action(p)
            return carry

        lax.fori_loop(chunk * per, (chunk + 1) * per, body, 0)

    def first(way, p):
        return copy(0, way, p, part.at[1 - way, span(p)], first_in.at[way, span(p)])

    def direct(way, p):
        return copy(1, way, p, part.at[2 + way, span(p)], direct_in.at[way, span(p)])

    def summed(way, p):
        return copy(2, way, p, part.at[4 + way, span(p)], sum_in.at[way, span(p)])

    def result(way, p, owner):
        return here_only(3, way, p, y_ref.at[span(p), columns(owner, 0, 2 * half)])

    def passed_on(way, p, owner):
        return here_only(4, way, p, y_ref.at[span(p), columns(owner, way, half)])

    def project_out(chunk, k0, k1):
        which = pl.ds(pl.multiple_of(chunk * rows, rows), rows)

        def body(n, carry):
            k, t = n // tiles, lax.rem(n, tiles)
            slot = lax.rem(k + blocks - bufs, bufs)

            @pl.when((chunk == 0) & (t == 0))
            def _():
                weights_here(slot)

            part[k, which, pl.ds(pl.multiple_of(t * width, width), width)] = jnp.dot(att_ref[which, :], pool[slot, pl.ds(pl.multiple_of(t * inner, inner), inner), :], preferred_element_type=F32)
            return carry

        lax.fori_loop(k0 * tiles, k1 * tiles, body, 0)

    def send_parts(chunk):
        def go(k, carry):
            project_out(chunk, k, k + 1)

            @pl.when(k == 0)
            def _():
                pieces_of(chunk, lambda p: first(1, p).start())

            @pl.when(k == 1)
            def _():
                pieces_of(chunk, lambda p: first(0, p).start())

            @pl.when(k == 3)
            def _():
                def both(p):
                    direct(0, p).start()
                    direct(1, p).start()

                pieces_of(chunk, both)

            return carry

        lax.fori_loop(0, 8, go, 0)

    def forward_sums(chunk):
        def action(p):
            for way in (0, 1):
                first(way, p).wait_recv()
                part[4 + way, span(p)] += first_in[way, span(p)]
                summed(way, p).start()

        pieces_of(chunk, action)

    def finish(chunk):
        def action(p):
            for way in (0, 1):
                direct(way, p).wait_recv()
                summed(way, p).wait_recv()
            for which in (0, 1):
                total = part[6 + which, span(p)] + sum_in[1 - which, span(p)] + direct_in[which, span(p)]
                total = total + x_ref[span(p), columns(me, which, half)].astype(F32)
                y_ref[span(p), columns(me, which, half)] = total.astype(BF16)
            for way in (0, 1):
                result(way, p, me).start()

        pieces_of(chunk, action)

    def forward_results(chunk):
        def action(p):
            for way, source in ((0, left), (1, right)):
                result(way, p, source).wait_recv()
                passed_on(way, p, source).start()

        pieces_of(chunk, action)

    def pipeline(stage, carry):
        @pl.when(stage < CHUNKS)
        def _():
            attend(stage)

        @pl.when(stage >= 1)
        def _():
            finish(stage - 1)

        @pl.when(stage < CHUNKS)
        def _():
            send_parts(stage)

        @pl.when(stage >= 1)
        def _():
            forward_results(stage - 1)

        @pl.when(stage < CHUNKS)
        def _():
            forward_sums(stage)

        return carry

    lax.fori_loop(0, CHUNKS + 1, pipeline, 0)

    def last(p, carry):
        for way in (0, 1):
            passed_on(way, p, far).wait_recv()
        pltpu.make_async_copy(y_ref.at[span(p)], y_hbm.at[span(p)], y_sem).start()
        return carry

    lax.fori_loop(0, PIECES, last, 0)

    def sent(p, carry):
        for way, source in ((0, left), (1, right)):
            first(way, p).wait_send()
            direct(way, p).wait_send()
            summed(way, p).wait_send()
            result(way, p, me).wait_send()
            passed_on(way, p, source).wait_send()
        return carry

    lax.fori_loop(0, PIECES, sent, 0)
    ring(own, own, 0, x_right).wait_send()
    ring(own, own, 1, x_left).wait_send()
    ring(kv_all.at[x_left, 0], kv_all.at[x_left, 0], 2, x_right).wait_send()
    ring(kv_all.at[x_right, 1], kv_all.at[x_right, 1], 3, x_left).wait_send()
    for index, slot in enumerate((here, x_left, x_right, x_far)):
        pair(slot, index).wait_send()
    pltpu.make_async_copy(y_ref, y_hbm, y_sem).wait()


def solution(mesh):
    n_ctx, n_tp = mesh.shape['ctx'], mesh.shape['tp']
    row_axes = ('dp', 'ctx')
    vmem = pl.BlockSpec(memory_space=pltpu.VMEM)
    hbm = pl.BlockSpec(memory_space=pl.ANY)
    dma = pltpu.SemaphoreType.DMA

    def device_step(hidden, w_q, w_k, w_v, w_o, k_prefix, v_prefix, k_suffix, v_suffix, seq_lens):
        seqs, model = hidden.shape
        positions, kv_heads, dim = k_prefix.shape
        slots = k_suffix.shape[1] * kv_heads
        inner = w_q.shape[1]
        group = inner // (kv_heads * dim)
        width = w_k.shape[1]
        half = model // (2 * n_tp)
        rows = seqs // CHUNKS
        size = min(PREFIX, rows)
        return pl.pallas_call(
            functools.partial(layer_kernel, dim ** -0.5, n_ctx, n_tp),
            name='layer',
            out_shape=jax.ShapeDtypeStruct((seqs, model), BF16),
            in_specs=[pl.BlockSpec(memory_space=pltpu.SMEM), vmem, vmem] + [hbm] * 7,
            out_specs=hbm,
            scratch_shapes=[
                pltpu.VMEM((seqs, model), BF16),
                pltpu.VMEM((seqs, model), BF16),
                pltpu.VMEM((8, model, width), BF16),
                pltpu.VMEM((n_ctx, 2, kv_heads, positions, dim), BF16),
                pltpu.VMEM((kv_heads, seqs * group, dim), F32),
                pltpu.VMEM((2, kv_heads, seqs, dim), F32),
                pltpu.VMEM((DEPTH, SUB, slots, dim), BF16),
                pltpu.VMEM((DEPTH, SUB, slots, dim), BF16),
                pltpu.VMEM((kv_heads, rows * group, dim), F32),
                pltpu.VMEM((kv_heads, rows * group, 1), F32),
                pltpu.VMEM((kv_heads, rows * group, 1), F32),
                pltpu.VMEM((size * group, dim), F32),
                pltpu.VMEM((seqs, inner), BF16),
                pltpu.VMEM((8, seqs, half), F32),
                pltpu.VMEM((2, seqs, half), F32),
                pltpu.VMEM((2, seqs, half), F32),
                pltpu.VMEM((2, seqs, half), F32),
                dma, dma, dma((8,)), dma((DEPTH,)), dma((DEPTH,)), dma((4,)), dma((4,)), dma((4,)), dma((4,)), dma((5, 2, PIECES)), dma((5, 2, PIECES)),
            ],
            compiler_params=pltpu.CompilerParams(collective_id=0, has_side_effects=True, vmem_limit_bytes=67000000),
        )(seq_lens, k_prefix.reshape(positions * kv_heads, dim), v_prefix.reshape(positions * kv_heads, dim), hidden, w_q, w_k, w_v, w_o, k_suffix.reshape(seqs, slots, dim), v_suffix.reshape(seqs, slots, dim))

    spec_in = (P(row_axes, None), P(None, 'tp'), P(None, 'tp'), P(None, 'tp'), P('tp', None), P(row_axes, 'tp', None), P(row_axes, 'tp', None), P(row_axes, None, 'tp', None), P(row_axes, None, 'tp', None), P(row_axes))
    return jax.shard_map(device_step, mesh=mesh, in_specs=spec_in, out_specs=P(row_axes, None), check_vma=False)
```
